32 devices in a mesh: row: 16 (over z, y, core), col: 2 (over x).
Axes of the slice: x: 2, y: 2, z: 4, core: 2. Of those that a mesh axis runs over, the one named last changes fastest.
Arguments:
- vectors: float32 [1024, 32768], P(('row', 'col')), may hold values from -6 to 6
- reflectors: float32 [6, 128, 32768], P(None, 'col', 'row')
- factors: float32 [6, 128, 128], replicated, as said below
Outputs:
- transformed: float32 [1024, 32768], P('col', 'row')
The draws below stay inside these ranges and needn't reach their ends.
Inputs may be any that keep to these rules, and one draw needn't show every extreme that they name: factors[k] is upper triangular, and its inverse equals the strict upper part of reflectors[k] reflectors[k]^T plus half of that product's diagonal, so each panel is orthogonal.
All inputs are finite; a program needn't handle non-finite values.
Results may differ from the reference program's by a relative error of at most 0.0001.
Values sent between devices are 32-bit elements; how exact they have to be, the bound alone decides.
No kernel may reach another device: no remote copies, remote signals or barrier semaphores. Data moves between devices by JAX's collectives and lax.ppermute only.
A program may use at most 128 MiB of HBM per device.

```python
import jax
import jax.numpy as jnp
from jax import lax

N = 32768
BLOCK = 128
PANELS = 6
EIGVECS = 1024


def invert_upper(matrix):
    identity = jnp.eye(matrix.shape[0], dtype=jnp.float32)
    return jax.scipy.linalg.solve_triangular(matrix, identity, lower=False)


def reflector_pair(key):
    random_part = jax.random.normal(jax.random.fold_in(key, 11), (PANELS, BLOCK, N), jnp.float32) / jnp.sqrt(jnp.float32(N))
    mixing = jnp.eye(BLOCK, dtype=jnp.float32) + 0.35 / jnp.sqrt(jnp.float32(BLOCK)) * jax.random.normal(jax.random.fold_in(key, 12), (PANELS, BLOCK, BLOCK), jnp.float32)
    reflect = jnp.einsum('pij,pjn->pin', mixing, random_part, precision=lax.Precision.HIGHEST)
    gram_matrix = jnp.einsum('pin,pjn->pij', reflect, reflect, precision=lax.Precision.HIGHEST)
    diagonal_half = 0.5 * jnp.einsum('pii->pi', gram_matrix)
    inverse = jnp.triu(gram_matrix, 1) + jax.vmap(jnp.diag)(diagonal_half)
    triangle = jax.vmap(invert_upper)(inverse)
    return (reflect, triangle)


def draw_reflectors(key, part):
    return reflector_pair(jax.random.fold_in(key, 7))[0]


def draw_factors(key, part):
    return reflector_pair(jax.random.fold_in(key, 7))[1]


def levels(own_key, extent, cuts, low, largest):
    gain = 1.0
    for position, shards_of in cuts:
        steps = jax.random.uniform(jax.random.fold_in(jax.random.fold_in(own_key, 6), position), (shards_of,), jnp.float32, low / len(cuts), largest / len(cuts))
        gain = gain * jnp.repeat(jnp.exp(steps), extent[position] // shards_of).reshape((-1,) + (1,) * (len(extent) - 1 - position))
    return gain


def gaussian(rng, extent, width, limit, pieces=(), kind=jnp.bfloat16):
    result = jax.random.normal(rng, extent, jnp.float32) * width
    if len(pieces) > 0:
        result = levels(rng, extent, pieces, -0.22, 0.18) * result
    return jnp.clip(result, min=-limit, max=limit).astype(kind)


def setup_inputs(seed: int = 0) -> dict:
    keys = jax.random.split(jax.random.key(seed), 4)
    return {
        "vectors": gaussian(keys[0], (EIGVECS, N), 1.0, 6.0, ((0, 32),), jnp.float32),
        "reflectors": draw_reflectors(jax.random.fold_in(keys[3], 71), 0),
        "factors": draw_factors(jax.random.fold_in(keys[3], 71), 0),
    }


def reference(vectors, reflectors, factors):
    current = vectors
    for panel in range(PANELS - 1, -1, -1):
        stacked = reflectors[panel]
        projection = lax.dot_general(current.astype(jnp.float32), stacked.astype(jnp.float32), (((1,), (1,)), ((), ())), precision=lax.Precision.HIGHEST, preferred_element_type=jnp.float32)
        update = jnp.dot(projection.astype(jnp.float32), factors[panel].T.astype(jnp.float32), precision=lax.Precision.HIGHEST, preferred_element_type=jnp.float32)
        current = current - jnp.dot(update.astype(jnp.float32), stacked.astype(jnp.float32), precision=lax.Precision.HIGHEST, preferred_element_type=jnp.float32)
    return current
```

```python
import functools

import jax
import jax.numpy as jnp
from jax import lax
from jax.experimental import pallas as pl
from jax.experimental.pallas import tpu as pltpu
from jax.sharding import PartitionSpec as P


LOW_BITS = 2
TILE = 512
PROJECT_TILE = 1024


def outside(value):
    return pltpu.with_memory_space_constraint(value, pltpu.HBM)


def halves(value):
    high = value.astype(jnp.bfloat16)
    return high, (value - high.astype(jnp.float32)).astype(jnp.bfloat16)


def cut_kernel(length, flips, where_ref, source_ref, *refs):
    count = len(flips)
    outs, (held_ref, in_sem, out_sem) = refs[:count], refs[count:]
    loads = []
    for index in range(count):
        start = pl.multiple_of((where_ref[0] ^ flips[index]) * length, length)
        load = pltpu.make_async_copy(source_ref.at[:, pl.ds(start, length)], held_ref.at[index], in_sem.at[index])
        load.start()
        loads.append(load)
    stores = []
    for index in range(count):
        loads[index].wait()
        store = pltpu.make_async_copy(held_ref.at[index], outs[index], out_sem.at[index])
        store.start()
        stores.append(store)
    for store in stores:
        store.wait()


def cut(where, vectors, flips, length):
    rows, count = vectors.shape[0], len(flips)
    return pl.pallas_call(
        functools.partial(cut_kernel, length, flips),
        out_shape=[jax.ShapeDtypeStruct((rows, length), jnp.float32)] * count,
        grid_spec=pltpu.PrefetchScalarGridSpec(
            num_scalar_prefetch=1,
            grid=(),
            in_specs=[pl.BlockSpec(memory_space=pl.ANY)],
            out_specs=[pl.BlockSpec(memory_space=pl.ANY)] * count,
            scratch_shapes=[
                pltpu.VMEM((count, rows, length), jnp.float32),
                pltpu.SemaphoreType.DMA((count,)),
                pltpu.SemaphoreType.DMA((count,)),
            ],
        ),
        cost_estimate=pl.CostEstimate(
            flops=count * rows * length * 100, bytes_accessed=8 * count * rows * length, transcendentals=0
        ),
        compiler_params=pltpu.CompilerParams(vmem_limit_bytes=8 << 20),
        name="cut",
    )(where, vectors)


def across(left, right):
    return lax.dot_general(left, right, (((1,), (1,)), ((), ())), preferred_element_type=jnp.float32)


def prepare_kernel(plan, col_of, where_ref, *refs):
    col_count, width, steps = plan
    parts, (high_ref, low_ref, packed_ref, total_ref) = refs[:col_count], refs[col_count:]
    count, own_width = parts[0].shape[:2]
    col = col_of(where_ref[0])
    own_high, own_low = [], []
    for flip, part in enumerate(parts):
        for panel in range(count):
            high, low = halves(part[panel])
            start = pl.multiple_of(panel * width + (col ^ flip) * own_width, own_width)
            high_ref[pl.ds(start, own_width), :] = high
            low_ref[pl.ds(start, own_width), :] = low
            if flip == 0 and panel:
                own_high.append(high)
                own_low.append(low)
    own_high, own_low = jnp.concatenate(own_high, axis=0), jnp.concatenate(own_low, axis=0)
    before = (count - 1) * width
    value = across(own_high, high_ref[:before, :])
    value += across(own_high, low_ref[:before, :])
    value += across(own_low, high_ref[:before, :])

    @pl.when(pl.program_id(0) == 0)
    def _():
        total_ref[...] = value

    @pl.when(pl.program_id(0) > 0)
    def _():
        total_ref[...] += value

    @pl.when(pl.program_id(0) == steps - 1)
    def _():
        index = 0
        for second in range(1, count):
            for first in range(second):
                rows = slice((second - 1) * own_width, second * own_width)
                packed_ref[index * own_width : (index + 1) * own_width, :] = total_ref[
                    rows, first * width : (first + 1) * width
                ]
                index += 1
        packed_ref[index * own_width :, :] = jnp.zeros_like(packed_ref[index * own_width :, :])


def prepare(where, col_of, parts, packed_rows):
    count, own_width, length = parts[0].shape
    width = own_width * len(parts)
    tile = min(TILE, length)
    steps = length // tile
    return pl.pallas_call(
        functools.partial(prepare_kernel, (len(parts), width, steps), col_of),
        out_shape=[
            pltpu.HBM((count * width, length), jnp.bfloat16),
            pltpu.HBM((count * width, length), jnp.bfloat16),
            jax.ShapeDtypeStruct((packed_rows, width), jnp.float32),
        ],
        grid_spec=pltpu.PrefetchScalarGridSpec(
            num_scalar_prefetch=1,
            grid=(steps,),
            in_specs=[pl.BlockSpec((count, own_width, tile), lambda i, where: (0, 0, i)) for _ in parts],
            out_specs=[
                pl.BlockSpec((count * width, tile), lambda i, where: (0, i)),
                pl.BlockSpec((count * width, tile), lambda i, where: (0, i)),
                pl.BlockSpec((packed_rows, width), lambda i, where: (0, 0)),
            ],
            scratch_shapes=[pltpu.VMEM(((count - 1) * own_width, (count - 1) * width), jnp.float32)],
        ),
        cost_estimate=pl.CostEstimate(
            flops=6 * (count - 1) ** 2 * own_width * width * length,
            bytes_accessed=8 * count * width * length,
            transcendentals=0,
        ),
        compiler_params=pltpu.CompilerParams(vmem_limit_bytes=32 << 20),
        name="prepare",
    )(where, *[outside(part) for part in parts])


def project_kernel(plan, shift_of, where_ref, *refs):
    n_groups, n_rest, col_count, n_added, n_out, steps = plan
    pieces, refs = refs[: n_groups * n_rest], refs[n_groups * n_rest :]
    (high_ref, low_ref), added, refs = refs[:2], refs[2 : 2 + n_added], refs[2 + n_added :]
    outs, chosen, total_ref = refs[:n_out], refs[n_out:-1], refs[-1]
    shift = shift_of(where_ref[0])
    values = [piece[...] for piece in pieces]
    for group in range(n_groups):
        for flip in range(col_count):
            target = chosen[group * col_count + flip]
            for block in range(n_rest // col_count):
                value = values[group * n_rest + block]
                for high in range(1, col_count):
                    other = values[group * n_rest + high * (n_rest // col_count) + block]
                    value = jnp.where((shift ^ flip) == high, other, value)
                target[block] = value
    high, low = halves(jnp.concatenate(values, axis=0))
    size = high.shape[0]
    both = across(jnp.concatenate([high, low], axis=0), high_ref[...])
    value = both[:size] + both[size:] + across(high, low_ref[...])

    @pl.when(pl.program_id(0) == 0)
    def _():
        total_ref[...] = value

    @pl.when(pl.program_id(0) > 0)
    def _():
        total_ref[...] += value

    @pl.when(pl.program_id(0) == steps - 1)
    def _():
        share = size // n_out
        for index, out in enumerate(outs):
            result = total_ref[index * share : (index + 1) * share, :]
            for ref in added:
                result = result + ref[index * share : (index + 1) * share, :]
            out[...] = result


def project(where, shift_of, groups, high, low, added, col_count, n_out):
    pieces = [piece for group in groups for piece in group]
    n_rest = len(groups[0])
    rows, length = pieces[0].shape
    total = high.shape[0]
    tile = min(PROJECT_TILE, length)
    steps = length // tile
    size = len(pieces) * rows
    blocks = n_rest // col_count
    fixed = lambda i, where: (0, 0)
    moving = lambda i, where: (0, i)
    outs = pl.pallas_call(
        functools.partial(project_kernel, (len(groups), n_rest, col_count, len(added), n_out, steps), shift_of),
        out_shape=[jax.ShapeDtypeStruct((size // n_out, total), jnp.float32)] * n_out
        + [pltpu.HBM((blocks, rows, length), jnp.float32)] * (len(groups) * col_count),
        grid_spec=pltpu.PrefetchScalarGridSpec(
            num_scalar_prefetch=1,
            grid=(steps,),
            in_specs=[pl.BlockSpec((rows, tile), moving) for _ in pieces]
            + [pl.BlockSpec((total, tile), moving)] * 2
            + [pl.BlockSpec(value.shape, fixed) for value in added],
            out_specs=[pl.BlockSpec((size // n_out, total), fixed)] * n_out
            + [pl.BlockSpec((blocks, rows, tile), lambda i, where: (0, 0, i))] * (len(groups) * col_count),
            scratch_shapes=[pltpu.VMEM((size, total), jnp.float32)],
        ),
        cost_estimate=pl.CostEstimate(
            flops=6 * size * total * length, bytes_accessed=4 * (2 * size + total) * length, transcendentals=0
        ),
        compiler_params=pltpu.CompilerParams(vmem_limit_bytes=32 << 20),
        name="project",
    )(where, *[outside(piece) for piece in pieces], outside(high), outside(low), *added)
    chosen = outs[n_out:]
    return outs[:n_out], [chosen[g * col_count : (g + 1) * col_count] for g in range(len(groups))]


def factor_kernel(pair_rows, crossed_ref, factor_ref, high_ref, low_ref, whole_ref):
    count, width = factor_ref.shape[:2]
    col_count = crossed_ref.shape[0]

    def dot(left, right, axis):
        return lax.dot_general(
            left,
            right,
            (((1,), (axis,)), ((), ())),
            precision=lax.Precision.HIGHEST,
            preferred_element_type=jnp.float32,
        )

    whole_ref[...] = jnp.zeros_like(whole_ref)
    eye = (
        lax.broadcasted_iota(jnp.int32, (width, width), 0) == lax.broadcasted_iota(jnp.int32, (width, width), 1)
    ).astype(jnp.float32)
    for first in reversed(range(count)):
        at = slice(first * width, (first + 1) * width)
        factor = factor_ref[first]
        whole_ref[at, at] = dot(eye, factor, 1)
        if first < count - 1:
            inner = []
            for second in range(first + 1, count):
                pair = second * (second - 1) // 2 + first
                for col in range(col_count):
                    inner.append(crossed_ref[col, pair * pair_rows : (pair + 1) * pair_rows, :])
            inner = jnp.concatenate(inner, axis=0)
            after = (first + 1) * width
            whole_ref[after:, at] = -dot(dot(whole_ref[after:, after:], inner, 0), factor, 1)
    high, low = halves(whole_ref[...])
    high_ref[...] = high
    low_ref[...] = low


def factor(crossed, factors, pair_rows):
    count, width = factors.shape[:2]
    shape = jax.ShapeDtypeStruct((count * width, count * width), jnp.bfloat16)
    return pl.pallas_call(
        functools.partial(factor_kernel, pair_rows),
        out_shape=[shape, shape],
        scratch_shapes=[pltpu.VMEM((count * width, count * width), jnp.float32)],
        cost_estimate=pl.CostEstimate(flops=width**3 * count**3 * 4, bytes_accessed=1 << 22, transcendentals=0),
        compiler_params=pltpu.CompilerParams(vmem_limit_bytes=16 << 20),
        name="factor",
    )(crossed, factors)


def update_kernel(plan, place_of, where_ref, *refs):
    n_given, n_vector, rows = plan
    given, refs = refs[:n_given], refs[n_given:]
    vectors, refs = refs[:n_vector], refs[n_vector:]
    factor_high, factor_low, reflect_high, reflect_low, out_ref, high_ref, low_ref = refs
    places = place_of(where_ref[0])

    @pl.when(pl.program_id(0) == 0)
    def _():
        index = 0
        for ref in given:
            for block in range(ref.shape[0]):
                high, low = halves(ref[block])
                start = pl.multiple_of(places[index] * rows, rows)
                high_ref[pl.ds(start, rows), :] = high
                low_ref[pl.ds(start, rows), :] = low
                index += 1
        high = high_ref[...]
        update = jnp.dot(high, factor_high[...], preferred_element_type=jnp.float32)
        update += jnp.dot(high, factor_low[...], preferred_element_type=jnp.float32)
        update += jnp.dot(low_ref[...], factor_high[...], preferred_element_type=jnp.float32)
        high_ref[...], low_ref[...] = halves(update)

    high = high_ref[...]
    total = jnp.dot(high, reflect_high[...], preferred_element_type=jnp.float32)
    total += jnp.dot(high, reflect_low[...], preferred_element_type=jnp.float32)
    total += jnp.dot(low_ref[...], reflect_high[...], preferred_element_type=jnp.float32)
    out_ref[...] = total
    index = sum(ref.shape[0] for ref in given)
    for ref in vectors:
        for block in range(ref.shape[0]):
            start = pl.multiple_of(places[index] * rows, rows)
            out_ref[pl.ds(start, rows), :] = ref[block] - out_ref[pl.ds(start, rows), :]
            index += 1


def apply_update(where, place_of, given, vectors, factor_parts, reflect_parts, rows):
    total, length = reflect_parts[0].shape
    count = sum(value.shape[0] for value in given)
    tile = min(TILE, length)
    specs = [pl.BlockSpec(value.shape, lambda i, where: (0, 0, 0)) for value in given]
    specs += [pl.BlockSpec((value.shape[0], rows, tile), lambda i, where: (0, 0, i)) for value in vectors]
    specs += [pl.BlockSpec((total, total), lambda i, where: (0, 0))] * 2
    specs += [pl.BlockSpec((total, tile), lambda i, where: (0, i))] * 2
    return pl.pallas_call(
        functools.partial(update_kernel, (len(given), len(vectors), rows), place_of),
        out_shape=jax.ShapeDtypeStruct((count * rows, length), jnp.float32),
        grid_spec=pltpu.PrefetchScalarGridSpec(
            num_scalar_prefetch=1,
            grid=(length // tile,),
            in_specs=specs,
            out_specs=pl.BlockSpec((count * rows, tile), lambda i, where: (0, i)),
            scratch_shapes=[pltpu.VMEM((count * rows, total), jnp.bfloat16)] * 2,
        ),
        cost_estimate=pl.CostEstimate(
            flops=6 * count * rows * total * length,
            bytes_accessed=4 * (2 * count * rows * length + total * length + count * rows * total),
            transcendentals=0,
        ),
        compiler_params=pltpu.CompilerParams(vmem_limit_bytes=40 << 20),
        name="apply_update",
    )(where, *given, *map(outside, vectors), *factor_parts, *map(outside, reflect_parts))


def flipped(value, amount, axis, size):
    return jnp.stack([lax.dynamic_index_in_dim(value, i ^ amount, axis, keepdims=False) for i in range(size)], axis)


def transform(vectors, reflectors, factors):
    rows, whole_length = vectors.shape
    row_count = lax.axis_size("row")
    col_count = lax.axis_size("col")
    length = whole_length // row_count
    count, own_width = reflectors.shape[:2]
    width = own_width * col_count
    per_col = row_count // col_count
    low_bits = min(LOW_BITS, per_col.bit_length() - 1)
    groups = 1 << low_bits
    middle = per_col // groups
    rest_count = col_count * middle
    row = lax.axis_index("row")
    col = lax.axis_index("col")
    where = (row * col_count + col)[None]

    def flip_row(value, bits):
        return lax.ppermute(value, "row", [(i, i ^ bits) for i in range(row_count)])

    def flip_col(value, bits):
        return lax.ppermute(value, "col", [(i, i ^ bits) for i in range(col_count)])

    reflects = [reflectors]
    for flip in range(1, col_count):
        reflects.append(flip_col(reflectors, flip))

    group_order = list(reversed(range(groups)))
    pieces = {}
    for low in group_order:
        flips = [rest * groups + low for rest in reversed(range(rest_count))]
        cuts = cut(row[None], vectors, flips, length)
        arrived = []
        for flip, piece in zip(flips, cuts):
            arrived.append(flip_row(piece, flip) if flip else piece)
        pieces[low] = arrived[::-1]

    pairs = count * (count - 1) // 2
    share = -(-pairs * own_width // (row_count * 8)) * 8
    reflect_high, reflect_low, packed = prepare(where, lambda w: w % col_count, reflects, share * row_count)
    packed = packed.reshape(row_count, share, width)
    for bit in range(low_bits):
        mine = (row >> bit) & 1
        split = packed.reshape(packed.shape[0] // 2, 2, share, width)
        sent = lax.dynamic_index_in_dim(split, 1 - mine, 1, keepdims=False)
        kept = lax.dynamic_index_in_dim(split, mine, 1, keepdims=False)
        packed = kept + flip_row(sent, 1 << bit)
    rest_of = row // groups
    total = lax.dynamic_index_in_dim(packed, rest_of, 0, keepdims=False)
    for flip in range(1, rest_count):
        total = total + flip_row(lax.dynamic_index_in_dim(packed, rest_of ^ flip, 0, keepdims=False), flip * groups)
    both = [total]
    for flip in range(1, col_count):
        both.append(flip_col(total, flip))
    total = flipped(jnp.stack(both), col, 0, col_count)
    spread = [total]
    for flip in range(1, rest_count):
        spread.append(flip_row(total, flip * groups))
    spread = flipped(jnp.stack(spread), rest_of, 0, rest_count)
    for bit in reversed(range(low_bits)):
        mine = (row >> bit) & 1
        other = flip_row(spread, 1 << bit)
        spread = jnp.where(mine == 0, jnp.stack([spread, other], 1), jnp.stack([other, spread], 1))
        spread = spread.reshape(-1, col_count, share, width)
    crossed = jnp.swapaxes(spread, 0, 1).reshape(col_count, row_count * share, width)
    factor_parts = factor(crossed, factors, own_width)

    def shift_of(w):
        return (w // col_count // per_col) ^ (w % col_count)

    chosen = {}
    added = {low: [] for low in group_order}
    half = max(groups // 2, 1)
    for part in range(0, groups, half):
        lows = group_order[part : part + half]
        sums, kept = project(
            where, shift_of, [pieces[low] for low in lows], reflect_high, reflect_low, [], col_count, half
        )
        for low, value, kept_here in zip(lows, sums, kept):
            chosen[low] = kept_here
            for other in added[low]:
                value = value + other
            if low:
                bit = low.bit_length() - 1
                added[low ^ (1 << bit)].append(flip_row(value, 1 << bit))
    sums = value.reshape(rest_count, rows, count * width)

    moved = {}
    for low in group_order:
        for flip in range(1, col_count):
            moved[low, flip] = flip_col(chosen[low][flip], flip)

    projection = 0.0
    for high_flip in range(col_count):
        for middle_flip in range(middle):
            pairs_of = []
            for source_row in range(row_count):
                for source_col in range(col_count):
                    high = source_row // per_col
                    inside = (source_row % per_col) ^ (middle_flip * groups)
                    target = (source_col * per_col + inside) * col_count + (high ^ high_flip)
                    pairs_of.append((source_row * col_count + source_col, target))
            projection = projection + lax.ppermute(sums[high_flip * middle + middle_flip], ("row", "col"), pairs_of)

    gathered = {}
    first_group = []
    for high_flip in range(col_count):
        for middle_flip in range(middle):
            flip = high_flip * per_col + middle_flip * groups
            first_group.append(flip_row(projection, flip) if flip else projection)
    gathered[0] = jnp.stack(first_group)
    for bit in reversed(range(low_bits)):
        for low in list(gathered):
            gathered[low | (1 << bit)] = flip_row(gathered[low], 1 << bit)

    order = list(range(groups))
    keys = [(low, 0) for low in order] + [(low, flip) for low in order for flip in range(1, col_count)]

    def place_of(where):
        row, col = where // col_count, where % col_count
        low_of, middle_of, high_of = row % groups, (row // groups) % middle, row // per_col
        places = []
        for low in order:
            for high_flip in range(col_count):
                for middle_flip in range(middle):
                    inside = (middle_of ^ middle_flip) * groups + (low_of ^ low)
                    places.append(inside * col_count + (high_of ^ high_flip))
        for low, flip in keys:
            for middle_flip in range(middle):
                inside = (middle_of ^ middle_flip) * groups + (low_of ^ low)
                places.append(inside * col_count + (col ^ flip))
        return places

    return apply_update(
        where,
        place_of,
        [gathered[low] for low in order],
        [chosen[low][0] if flip == 0 else moved[low, flip] for low, flip in keys],
        factor_parts,
        (reflect_high, reflect_low),
        rows,
    )


def solution(mesh):
    return jax.shard_map(
        transform,
        mesh=mesh,
        in_specs=(P(("row", "col"), None), P(None, "col", "row"), P()),
        out_specs=P("col", "row"),
        check_vma=False,
    )
```

```python
import functools

import jax
import jax.numpy as jnp
from jax import lax
from jax.experimental import pallas as pl
from jax.experimental.pallas import tpu as pltpu
from jax.sharding import PartitionSpec as P


LOW_BITS = 2
TILE = 512
PROJECT_TILE = 1024


def outside(value):
    return pltpu.with_memory_space_constraint(value, pltpu.HBM)


def halves(value):
    high = value.astype(jnp.bfloat16)
    return high, (value - high.astype(jnp.float32)).astype(jnp.bfloat16)


def cut_kernel(length, flips, where_ref, source_ref, *refs):
    count = len(flips)
    outs, (held_ref, in_sem, out_sem) = refs[:count], refs[count:]
    loads = []
    for index in range(count):
        start = pl.multiple_of((where_ref[0] ^ flips[index]) * length, length)
        load = pltpu.make_async_copy(source_ref.at[:, pl.ds(start, length)], held_ref.at[index], in_sem.at[index])
        load.start()
        loads.append(load)
    stores = []
    for index in range(count):
        loads[index].wait()
        store = pltpu.make_async_copy(held_ref.at[index], outs[index], out_sem.at[index])
        store.start()
        stores.append(store)
    for store in stores:
        store.wait()


def cut(where, vectors, flips, length):
    rows, count = vectors.shape[0], len(flips)
    return pl.pallas_call(
        functools.partial(cut_kernel, length, flips),
        out_shape=[jax.ShapeDtypeStruct((rows, length), jnp.float32)] * count,
        grid_spec=pltpu.PrefetchScalarGridSpec(
            num_scalar_prefetch=1,
            grid=(),
            in_specs=[pl.BlockSpec(memory_space=pl.ANY)],
            out_specs=[pl.BlockSpec(memory_space=pl.ANY)] * count,
            scratch_shapes=[
                pltpu.VMEM((count, rows, length), jnp.float32),
                pltpu.SemaphoreType.DMA((count,)),
                pltpu.SemaphoreType.DMA((count,)),
            ],
        ),
        cost_estimate=pl.CostEstimate(
            flops=count * rows * length * 100, bytes_accessed=8 * count * rows * length, transcendentals=0
        ),
        compiler_params=pltpu.CompilerParams(vmem_limit_bytes=8 << 20),
        name="cut",
    )(where, outside(vectors))


def across(left, right):
    return lax.dot_general(left, right, (((1,), (1,)), ((), ())), preferred_element_type=jnp.float32)


def prepare_kernel(plan, col_of, where_ref, *refs):
    col_count, width, steps = plan
    parts, (high_ref, low_ref, packed_ref, total_ref) = refs[:col_count], refs[col_count:]
    count, own_width = parts[0].shape[:2]
    col = col_of(where_ref[0])
    own_high, own_low = [], []
    for flip, part in enumerate(parts):
        for panel in range(count):
            high, low = halves(part[panel])
            start = pl.multiple_of(panel * width + (col ^ flip) * own_width, own_width)
            high_ref[pl.ds(start, own_width), :] = high
            low_ref[pl.ds(start, own_width), :] = low
            if flip == 0 and panel:
                own_high.append(high)
                own_low.append(low)
    own_high, own_low = jnp.concatenate(own_high, axis=0), jnp.concatenate(own_low, axis=0)
    before = (count - 1) * width
    value = across(own_high, high_ref[:before, :])
    value += across(own_high, low_ref[:before, :])
    value += across(own_low, high_ref[:before, :])

    @pl.when(pl.program_id(0) == 0)
    def _():
        total_ref[...] = value

    @pl.when(pl.program_id(0) > 0)
    def _():
        total_ref[...] += value

    @pl.when(pl.program_id(0) == steps - 1)
    def _():
        index = 0
        for second in range(1, count):
            for first in range(second):
                rows = slice((second - 1) * own_width, second * own_width)
                packed_ref[index * own_width : (index + 1) * own_width, :] = total_ref[
                    rows, first * width : (first + 1) * width
                ]
                index += 1
        packed_ref[index * own_width :, :] = jnp.zeros_like(packed_ref[index * own_width :, :])


def prepare(where, col_of, parts, packed_rows):
    count, own_width, length = parts[0].shape
    width = own_width * len(parts)
    tile = min(TILE, length)
    steps = length // tile
    return pl.pallas_call(
        functools.partial(prepare_kernel, (len(parts), width, steps), col_of),
        out_shape=[
            pltpu.HBM((count * width, length), jnp.bfloat16),
            pltpu.HBM((count * width, length), jnp.bfloat16),
            jax.ShapeDtypeStruct((packed_rows, width), jnp.float32),
        ],
        grid_spec=pltpu.PrefetchScalarGridSpec(
            num_scalar_prefetch=1,
            grid=(steps,),
            in_specs=[pl.BlockSpec((count, own_width, tile), lambda i, where: (0, 0, i)) for _ in parts],
            out_specs=[
                pl.BlockSpec((count * width, tile), lambda i, where: (0, i)),
                pl.BlockSpec((count * width, tile), lambda i, where: (0, i)),
                pl.BlockSpec((packed_rows, width), lambda i, where: (0, 0)),
            ],
            scratch_shapes=[pltpu.VMEM(((count - 1) * own_width, (count - 1) * width), jnp.float32)],
        ),
        cost_estimate=pl.CostEstimate(
            flops=6 * (count - 1) ** 2 * own_width * width * length,
            bytes_accessed=8 * count * width * length,
            transcendentals=0,
        ),
        compiler_params=pltpu.CompilerParams(vmem_limit_bytes=32 << 20),
        name="prepare",
    )(where, *[outside(part) for part in parts])


def project_kernel(plan, shift_of, where_ref, *refs):
    n_groups, n_rest, col_count, n_added, n_out, steps, choosing = plan
    pieces, refs = refs[: n_groups * n_rest], refs[n_groups * n_rest :]
    (high_ref, low_ref), added, refs = refs[:2], refs[2 : 2 + n_added], refs[2 + n_added :]
    outs, chosen, total_ref = refs[:n_out], refs[n_out:-1], refs[-1]
    shift = shift_of(where_ref[0])
    values = [piece[...] for piece in pieces]
    for group in range(n_groups if choosing else 0):
        for flip in range(col_count):
            target = chosen[group * col_count + flip]
            for block in range(n_rest // col_count):
                value = values[group * n_rest + block]
                for high in range(1, col_count):
                    other = values[group * n_rest + high * (n_rest // col_count) + block]
                    value = jnp.where((shift ^ flip) == high, other, value)
                target[block] = value
    high, low = halves(jnp.concatenate(values, axis=0))
    size = high.shape[0]
    both = across(jnp.concatenate([high, low], axis=0), high_ref[...])
    value = both[:size] + both[size:] + across(high, low_ref[...])

    @pl.when(pl.program_id(0) == 0)
    def _():
        total_ref[...] = value

    @pl.when(pl.program_id(0) > 0)
    def _():
        total_ref[...] += value

    @pl.when(pl.program_id(0) == steps - 1)
    def _():
        share = size // n_out
        for index, out in enumerate(outs):
            result = total_ref[index * share : (index + 1) * share, :]
            for ref in added:
                result = result + ref[index * share : (index + 1) * share, :]
            out[...] = result


def project(where, shift_of, groups, high, low, added, col_count, n_out, choosing):
    pieces = [piece for group in groups for piece in group]
    n_rest = len(groups[0])
    rows, length = pieces[0].shape
    total = high.shape[0]
    tile = min(PROJECT_TILE, length)
    steps = length // tile
    size = len(pieces) * rows
    blocks = n_rest // col_count
    n_chosen = len(groups) * col_count if choosing else 0
    fixed = lambda i, where: (0, 0)
    moving = lambda i, where: (0, i)
    outs = pl.pallas_call(
        functools.partial(project_kernel, (len(groups), n_rest, col_count, len(added), n_out, steps, choosing), shift_of),
        out_shape=[jax.ShapeDtypeStruct((size // n_out, total), jnp.float32)] * n_out
        + [pltpu.HBM((blocks, rows, length), jnp.float32)] * n_chosen,
        grid_spec=pltpu.PrefetchScalarGridSpec(
            num_scalar_prefetch=1,
            grid=(steps,),
            in_specs=[pl.BlockSpec((rows, tile), moving) for _ in pieces]
            + [pl.BlockSpec((total, tile), moving)] * 2
            + [pl.BlockSpec(value.shape, fixed) for value in added],
            out_specs=[pl.BlockSpec((size // n_out, total), fixed)] * n_out
            + [pl.BlockSpec((blocks, rows, tile), lambda i, where: (0, 0, i))] * n_chosen,
            scratch_shapes=[pltpu.VMEM((size, total), jnp.float32)],
        ),
        cost_estimate=pl.CostEstimate(
            flops=6 * size * total * length, bytes_accessed=4 * (2 * size + total) * length, transcendentals=0
        ),
        compiler_params=pltpu.CompilerParams(vmem_limit_bytes=32 << 20),
        name="project",
    )(where, *[outside(piece) for piece in pieces], outside(high), outside(low), *added)
    chosen = outs[n_out:]
    return outs[:n_out], [chosen[g * col_count : (g + 1) * col_count] for g in range(len(groups) if choosing else 0)]


def choose_kernel(col_count, shift_of, where_ref, *refs):
    chosen, (held_ref, in_sem, out_sem) = refs[-3 - col_count : -3], refs[-3:]
    pieces = refs[: -3 - col_count]
    blocks = len(pieces) // col_count
    shift = shift_of(where_ref[0])
    loads = [pltpu.make_async_copy(piece, held_ref.at[i], in_sem.at[i]) for i, piece in enumerate(pieces)]
    for load in loads:
        load.start()
    for load in loads:
        load.wait()
    stores = []
    for flip in range(col_count):
        for block in range(blocks):
            source = (shift ^ flip) * blocks + block
            stores.append(
                pltpu.make_async_copy(held_ref.at[source], chosen[flip].at[block], out_sem.at[len(stores)])
            )
    for store in stores:
        store.start()
    for store in stores:
        store.wait()


def choose(where, shift_of, pieces, col_count):
    rows, length = pieces[0].shape
    anywhere = pl.BlockSpec(memory_space=pltpu.HBM)
    return pl.pallas_call(
        functools.partial(choose_kernel, col_count, shift_of),
        out_shape=[pltpu.HBM((len(pieces) // col_count, rows, length), jnp.float32)] * col_count,
        grid_spec=pltpu.PrefetchScalarGridSpec(
            num_scalar_prefetch=1,
            grid=(),
            in_specs=[anywhere] * len(pieces),
            out_specs=[anywhere] * col_count,
            scratch_shapes=[
                pltpu.VMEM((len(pieces), rows, length), jnp.float32),
                pltpu.SemaphoreType.DMA((len(pieces),)),
                pltpu.SemaphoreType.DMA((len(pieces),)),
            ],
        ),
        cost_estimate=pl.CostEstimate(
            flops=1 << 28, bytes_accessed=8 * len(pieces) * rows * length, transcendentals=0
        ),
        compiler_params=pltpu.CompilerParams(vmem_limit_bytes=8 << 20),
        name="choose",
    )(where, *[outside(piece) for piece in pieces])


def factor_kernel(pair_rows, crossed_ref, factor_ref, high_ref, low_ref, whole_ref):
    count, width = factor_ref.shape[:2]
    col_count = crossed_ref.shape[0]

    def dot(left, right, axis):
        def once(first, second):
            return lax.dot_general(
                first, second, (((1,), (axis,)), ((), ())), preferred_element_type=jnp.float32
            )

        (left_high, left_low), (right_high, right_low) = halves(left), halves(right)
        return once(left_high, right_high) + once(left_high, right_low) + once(left_low, right_high)

    whole_ref[...] = jnp.zeros_like(whole_ref)
    for first in reversed(range(count)):
        at = slice(first * width, (first + 1) * width)
        factor = factor_ref[first]
        whole_ref[at, at] = factor.T
        if first < count - 1:
            inner = []
            for second in range(first + 1, count):
                pair = second * (second - 1) // 2 + first
                for col in range(col_count):
                    inner.append(crossed_ref[col, pair * pair_rows : (pair + 1) * pair_rows, :])
            inner = jnp.concatenate(inner, axis=0)
            after = (first + 1) * width
            whole_ref[after:, at] = -dot(dot(whole_ref[after:, after:], inner, 0), factor, 1)
    high, low = halves(whole_ref[...])
    high_ref[...] = high
    low_ref[...] = low


def factor(crossed, factors, pair_rows):
    count, width = factors.shape[:2]
    shape = jax.ShapeDtypeStruct((count * width, count * width), jnp.bfloat16)
    return pl.pallas_call(
        functools.partial(factor_kernel, pair_rows),
        out_shape=[shape, shape],
        scratch_shapes=[pltpu.VMEM((count * width, count * width), jnp.float32)],
        cost_estimate=pl.CostEstimate(flops=width**3 * count**3 * 4, bytes_accessed=1 << 22, transcendentals=0),
        compiler_params=pltpu.CompilerParams(vmem_limit_bytes=16 << 20),
        name="factor",
    )(crossed, factors)


def update_kernel(plan, place_of, where_ref, *refs):
    n_given, n_vector, n_before, rows = plan
    given, refs = refs[:n_given], refs[n_given:]
    vectors, refs = refs[:n_vector], refs[n_vector:]
    factor_high, factor_low, reflect_high, reflect_low = refs[:4]
    out_ref, high_ref, low_ref = refs[4 + n_before :]
    given_places, vector_places = place_of(where_ref[0])
    middle, _, inner, tile = out_ref.shape

    @pl.when(pl.program_id(0) == 0)
    def _():
        index = 0
        for ref in given:
            for block in range(ref.shape[0]):
                high, low = halves(ref[block])
                start = pl.multiple_of(given_places[index] * rows, rows)
                high_ref[pl.ds(start, rows), :] = high
                low_ref[pl.ds(start, rows), :] = low
                index += 1
        high = high_ref[...]
        update = jnp.dot(high, factor_high[...], preferred_element_type=jnp.float32)
        update += jnp.dot(high, factor_low[...], preferred_element_type=jnp.float32)
        update += jnp.dot(low_ref[...], factor_high[...], preferred_element_type=jnp.float32)
        high_ref[...], low_ref[...] = halves(update)

    high = high_ref[...]
    total = jnp.dot(high, reflect_high[...], preferred_element_type=jnp.float32)
    total += jnp.dot(high, reflect_low[...], preferred_element_type=jnp.float32)
    total += jnp.dot(low_ref[...], reflect_high[...], preferred_element_type=jnp.float32)
    out_ref[:, 0] = total.reshape(middle, inner, tile)
    index = 0
    for ref in vectors:
        for block in range(ref.shape[0]):
            outer, place = vector_places[index]
            at = (outer, 0, pl.ds(pl.multiple_of(place * rows, rows), rows))
            out_ref[at] = ref[block] - out_ref[at]
            index += 1


def apply_update(where, place_of, part_of, parts, middle, given, vectors, factor_parts, reflect_parts, before):
    total, length = reflect_parts[0].shape
    rows = vectors[0].shape[1]
    count = sum(value.shape[0] for value in given)
    inner = count * rows // middle
    tile = min(TILE, length)
    specs = [pl.BlockSpec(value.shape, lambda i, where: (0, 0, 0)) for value in given]
    specs += [pl.BlockSpec((value.shape[0], rows, tile), lambda i, where: (0, 0, i)) for value in vectors]
    specs += [pl.BlockSpec((total, total), lambda i, where: (0, 0))] * 2
    specs += [pl.BlockSpec((total, tile), lambda i, where: (0, i))] * 2
    specs += [pl.BlockSpec(memory_space=pltpu.HBM)] * len(before)
    return pl.pallas_call(
        functools.partial(update_kernel, (len(given), len(vectors), len(before), rows), place_of),
        out_shape=jax.ShapeDtypeStruct((middle, parts, inner, length), jnp.float32),
        grid_spec=pltpu.PrefetchScalarGridSpec(
            num_scalar_prefetch=1,
            grid=(length // tile,),
            in_specs=specs,
            out_specs=pl.BlockSpec((middle, 1, inner, tile), lambda i, where: (0, part_of(where[0]), 0, i)),
            scratch_shapes=[pltpu.VMEM((count * rows, total), jnp.bfloat16)] * 2,
        ),
        input_output_aliases={len(specs): 0} if before else {},
        cost_estimate=pl.CostEstimate(
            flops=6 * count * rows * total * length,
            bytes_accessed=4 * (2 * count * rows * length + total * length + count * rows * total),
            transcendentals=0,
        ),
        compiler_params=pltpu.CompilerParams(vmem_limit_bytes=40 << 20),
        name="apply_update",
    )(where, *given, *map(outside, vectors), *factor_parts, *map(outside, reflect_parts), *before)


def flipped(value, amount, axis, size):
    return jnp.stack([lax.dynamic_index_in_dim(value, i ^ amount, axis, keepdims=False) for i in range(size)], axis)


def transform(vectors, reflectors, factors):
    rows, whole_length = vectors.shape
    row_count = lax.axis_size("row")
    col_count = lax.axis_size("col")
    length = whole_length // row_count
    count, own_width = reflectors.shape[:2]
    width = own_width * col_count
    per_col = row_count // col_count
    low_bits = min(LOW_BITS, per_col.bit_length() - 1)
    groups = 1 << low_bits
    middle = per_col // groups
    rest_count = col_count * middle
    row = lax.axis_index("row")
    col = lax.axis_index("col")
    where = (row * col_count + col)[None]

    def flip_row(value, bits):
        return lax.ppermute(value, "row", [(i, i ^ bits) for i in range(row_count)])

    def flip_col(value, bits):
        return lax.ppermute(value, "col", [(i, i ^ bits) for i in range(col_count)])

    reflects = [reflectors]
    for flip in range(1, col_count):
        reflects.append(flip_col(reflectors, flip))

    group_order = list(reversed(range(groups)))
    pieces = {}
    for low in group_order:
        flips = [rest * groups + low for rest in reversed(range(rest_count))]
        cuts = cut(row[None], vectors, flips, length)
        arrived = []
        for flip, piece in zip(flips, cuts):
            arrived.append(flip_row(piece, flip) if flip else piece)
        pieces[low] = arrived[::-1]

    def shift_of(w):
        return (w // col_count // per_col) ^ (w % col_count)

    half = max(groups // 2, 1)
    chosen = {}
    for low in group_order:
        chosen[low] = choose(where, shift_of, pieces[low], col_count)

    pairs = count * (count - 1) // 2
    share = -(-pairs * own_width // (row_count * 8)) * 8
    reflect_high, reflect_low, packed = prepare(where, lambda w: w % col_count, reflects, share * row_count)
    packed = packed.reshape(row_count, share, width)
    for bit in range(low_bits):
        mine = (row >> bit) & 1
        split = packed.reshape(packed.shape[0] // 2, 2, share, width)
        sent = lax.dynamic_index_in_dim(split, 1 - mine, 1, keepdims=False)
        kept = lax.dynamic_index_in_dim(split, mine, 1, keepdims=False)
        packed = kept + flip_row(sent, 1 << bit)
    rest_of = row // groups
    total = lax.dynamic_index_in_dim(packed, rest_of, 0, keepdims=False)
    for flip in range(1, rest_count):
        total = total + flip_row(lax.dynamic_index_in_dim(packed, rest_of ^ flip, 0, keepdims=False), flip * groups)
    both = [total]
    for flip in range(1, col_count):
        both.append(flip_col(total, flip))
    total = flipped(jnp.stack(both), col, 0, col_count)
    spread = [total]
    for flip in range(1, rest_count):
        spread.append(flip_row(total, flip * groups))
    spread = flipped(jnp.stack(spread), rest_of, 0, rest_count)
    for bit in reversed(range(low_bits)):
        mine = (row >> bit) & 1
        other = flip_row(spread, 1 << bit)
        spread = jnp.where(mine == 0, jnp.stack([spread, other], 1), jnp.stack([other, spread], 1))
        spread = spread.reshape(-1, col_count, share, width)
    crossed = jnp.swapaxes(spread, 0, 1).reshape(col_count, row_count * share, width)
    factor_parts = factor(crossed, factors, own_width)

    added = {low: [] for low in group_order}
    for lows in [group_order[:half]] + [[low] for low in group_order[half:]]:
        sums, _ = project(
            where,
            shift_of,
            [pieces[low] for low in lows],
            reflect_high,
            reflect_low,
            [],
            col_count,
            len(lows),
            False,
        )
        for low, value in zip(lows, sums):
            for other in added[low]:
                value = value + other
            if low:
                bit = low.bit_length() - 1
                added[low ^ (1 << bit)].append(flip_row(value, 1 << bit))
    value = value.reshape(col_count, middle, rows, count * width)
    step = middle // 2
    while step:
        value = value[:, :step] + flip_row(value[:, step:], step * groups)
        step //= 2
    sums = value[:, 0]

    moved = {}
    for low in group_order:
        for flip in range(1, col_count):
            moved[low, flip] = flip_col(chosen[low][flip], flip)

    projection = 0.0
    for high_flip in range(col_count):
        pairs_of = []
        for source_row in range(row_count):
            for source_col in range(col_count):
                high, inside = source_row // per_col, source_row % per_col
                target = (source_col * per_col + inside) * col_count + (high ^ high_flip)
                pairs_of.append((source_row * col_count + source_col, target))
        projection = projection + lax.ppermute(sums[high_flip], ("row", "col"), pairs_of)

    gathered = {}
    first_group = []
    for high_flip in range(col_count):
        for middle_flip in range(middle):
            flip = high_flip * per_col + middle_flip * groups
            first_group.append(flip_row(projection, flip) if flip else projection)
    gathered[0] = first_group
    for bit in reversed(range(low_bits)):
        for low in list(gathered):
            blocks = gathered[low]
            target = low | (1 << bit)
            if bit:
                sent = []
                for block in blocks:
                    sent.append(flip_row(block, 1 << bit))
                gathered[target] = sent
            else:
                gathered[target] = [flip_row(jnp.stack(blocks), 1)]
    gathered = {low: [b.reshape(-1, rows, count * width) for b in blocks] for low, blocks in gathered.items()}

    parts = 1
    per_part = groups // parts

    def place_of(lows):
        def places(where):
            row, col = where // col_count, where % col_count
            low_of, middle_of, high_of = row % groups, (row // groups) % middle, row // per_col
            given_places, vector_places = [], []
            for low in lows:
                inside = (low_of ^ low) % per_part
                for high_flip in range(col_count):
                    for middle_flip in range(middle):
                        given_places.append(
                            ((middle_of ^ middle_flip) * per_part + inside) * col_count + (high_of ^ high_flip)
                        )
            for flip in range(col_count):
                for low in lows:
                    inside = (low_of ^ low) % per_part
                    for middle_flip in range(middle):
                        vector_places.append((middle_of ^ middle_flip, inside * col_count + (col ^ flip)))
            return given_places, vector_places

        return places

    before = ()
    for part in range(parts):
        lows = list(range(part * per_part, (part + 1) * per_part))
        result = apply_update(
            where,
            place_of(lows),
            lambda w, part=part: ((w // col_count) % groups) // per_part ^ part,
            parts,
            middle,
            [block for low in lows for block in gathered[low]],
            [chosen[low][0] if flip == 0 else moved[low, flip] for flip in range(col_count) for low in lows],
            factor_parts,
            (reflect_high, reflect_low),
            before,
        )
        before = (result,)
    return result.reshape(row_count * rows, length)


def solution(mesh):
    return jax.shard_map(
        transform,
        mesh=mesh,
        in_specs=(P(("row", "col"), None), P(None, "col", "row"), P()),
        out_specs=P("col", "row"),
        check_vma=False,
    )
```

```python
import functools

import jax
import jax.numpy as jnp
from jax import lax
from jax.experimental import pallas as pl
from jax.experimental.pallas import tpu as pltpu
from jax.sharding import PartitionSpec as P


LOW_BITS = 2
TILE = 512
PROJECT_TILE = 1024


def outside(value):
    return pltpu.with_memory_space_constraint(value, pltpu.HBM)


def chunked(total, step):
    return [slice(start, min(start + step, total)) for start in range(0, total, step)]


def halves(value):
    high = value.astype(jnp.bfloat16)
    return high, (value - high.astype(jnp.float32)).astype(jnp.bfloat16)


def cut_kernel(length, flips, where_ref, source_ref, *refs):
    count = len(flips)
    outs, (held_ref, in_sem, out_sem) = refs[:count], refs[count:]
    loads = []
    for index in range(count):
        start = pl.multiple_of((where_ref[0] ^ flips[index]) * length, length)
        load = pltpu.make_async_copy(source_ref.at[:, pl.ds(start, length)], held_ref.at[index], in_sem.at[index])
        load.start()
        loads.append(load)
    stores = []
    for index in range(count):
        loads[index].wait()
        store = pltpu.make_async_copy(held_ref.at[index], outs[index], out_sem.at[index])
        store.start()
        stores.append(store)
    for store in stores:
        store.wait()


def cut(where, vectors, flips, length):
    rows, count = vectors.shape[0], len(flips)
    return pl.pallas_call(
        functools.partial(cut_kernel, length, flips),
        out_shape=[jax.ShapeDtypeStruct((rows, length), jnp.float32)] * count,
        grid_spec=pltpu.PrefetchScalarGridSpec(
            num_scalar_prefetch=1,
            grid=(),
            in_specs=[pl.BlockSpec(memory_space=pl.ANY)],
            out_specs=[pl.BlockSpec(memory_space=pl.ANY)] * count,
            scratch_shapes=[
                pltpu.VMEM((count, rows, length), jnp.float32),
                pltpu.SemaphoreType.DMA((count,)),
                pltpu.SemaphoreType.DMA((count,)),
            ],
        ),
        cost_estimate=pl.CostEstimate(
            flops=count * rows * length * 100, bytes_accessed=8 * count * rows * length, transcendentals=0
        ),
        compiler_params=pltpu.CompilerParams(vmem_limit_bytes=8 << 20),
        name="cut",
    )(where, outside(vectors))


def across(left, right):
    return lax.dot_general(left, right, (((1,), (1,)), ((), ())), preferred_element_type=jnp.float32)


def prepare_kernel(plan, col_of, where_ref, *refs):
    col_count, width, steps = plan
    parts, (high_ref, low_ref, packed_ref, total_ref) = refs[:col_count], refs[col_count:]
    count, own_width = parts[0].shape[:2]
    col = col_of(where_ref[0])
    own_high, own_low = [], []
    for flip, part in enumerate(parts):
        for panel in range(count):
            high, low = halves(part[panel])
            start = pl.multiple_of(panel * width + (col ^ flip) * own_width, own_width)
            high_ref[pl.ds(start, own_width), :] = high
            low_ref[pl.ds(start, own_width), :] = low
            if flip == 0 and panel:
                own_high.append(high)
                own_low.append(low)
    own_high, own_low = jnp.concatenate(own_high, axis=0), jnp.concatenate(own_low, axis=0)
    before = (count - 1) * width
    value = across(own_high, high_ref[:before, :])
    value += across(own_high, low_ref[:before, :])
    value += across(own_low, high_ref[:before, :])

    @pl.when(pl.program_id(0) == 0)
    def _():
        total_ref[...] = value

    @pl.when(pl.program_id(0) > 0)
    def _():
        total_ref[...] += value

    @pl.when(pl.program_id(0) == steps - 1)
    def _():
        index = 0
        for second in range(1, count):
            for first in range(second):
                rows = slice((second - 1) * own_width, second * own_width)
                packed_ref[index * own_width : (index + 1) * own_width, :] = total_ref[
                    rows, first * width : (first + 1) * width
                ]
                index += 1
        packed_ref[index * own_width :, :] = jnp.zeros_like(packed_ref[index * own_width :, :])


def prepare(where, col_of, parts, packed_rows):
    count, own_width, length = parts[0].shape
    width = own_width * len(parts)
    tile = min(TILE, length)
    steps = length // tile
    return pl.pallas_call(
        functools.partial(prepare_kernel, (len(parts), width, steps), col_of),
        out_shape=[
            pltpu.HBM((count * width, length), jnp.bfloat16),
            pltpu.HBM((count * width, length), jnp.bfloat16),
            jax.ShapeDtypeStruct((packed_rows, width), jnp.float32),
        ],
        grid_spec=pltpu.PrefetchScalarGridSpec(
            num_scalar_prefetch=1,
            grid=(steps,),
            in_specs=[pl.BlockSpec((count, own_width, tile), lambda i, where: (0, 0, i)) for _ in parts],
            out_specs=[
                pl.BlockSpec((count * width, tile), lambda i, where: (0, i)),
                pl.BlockSpec((count * width, tile), lambda i, where: (0, i)),
                pl.BlockSpec((packed_rows, width), lambda i, where: (0, 0)),
            ],
            scratch_shapes=[pltpu.VMEM(((count - 1) * own_width, (count - 1) * width), jnp.float32)],
        ),
        cost_estimate=pl.CostEstimate(
            flops=6 * (count - 1) ** 2 * own_width * width * length,
            bytes_accessed=8 * count * width * length,
            transcendentals=0,
        ),
        compiler_params=pltpu.CompilerParams(vmem_limit_bytes=32 << 20),
        name="prepare",
    )(where, *[outside(part) for part in parts])


def project_kernel(plan, shift_of, where_ref, *refs):
    n_groups, n_rest, col_count, n_added, n_out, steps, choosing = plan
    pieces, refs = refs[: n_groups * n_rest], refs[n_groups * n_rest :]
    (high_ref, low_ref), added, refs = refs[:2], refs[2 : 2 + n_added], refs[2 + n_added :]
    outs, chosen, total_ref = refs[:n_out], refs[n_out:-1], refs[-1]
    shift = shift_of(where_ref[0])
    values = [piece[...] for piece in pieces]
    for group in range(n_groups if choosing else 0):
        for flip in range(col_count):
            target = chosen[group * col_count + flip]
            for block in range(n_rest // col_count):
                value = values[group * n_rest + block]
                for high in range(1, col_count):
                    other = values[group * n_rest + high * (n_rest // col_count) + block]
                    value = jnp.where((shift ^ flip) == high, other, value)
                target[block] = value
    high, low = halves(jnp.concatenate(values, axis=0))
    size = high.shape[0]
    both = across(jnp.concatenate([high, low], axis=0), high_ref[...])
    value = both[:size] + both[size:] + across(high, low_ref[...])

    @pl.when(pl.program_id(0) == 0)
    def _():
        total_ref[...] = value

    @pl.when(pl.program_id(0) > 0)
    def _():
        total_ref[...] += value

    @pl.when(pl.program_id(0) == steps - 1)
    def _():
        share = size // n_out
        for index, out in enumerate(outs):
            result = total_ref[index * share : (index + 1) * share, :]
            for ref in added:
                result = result + ref[index * share : (index + 1) * share, :]
            out[...] = result


def project(where, shift_of, groups, high, low, added, col_count, n_out, choosing):
    pieces = [piece for group in groups for piece in group]
    n_rest = len(groups[0])
    rows, length = pieces[0].shape
    total = high.shape[0]
    tile = min(PROJECT_TILE, length)
    steps = length // tile
    size = len(pieces) * rows
    blocks = n_rest // col_count
    n_chosen = len(groups) * col_count if choosing else 0
    fixed = lambda i, where: (0, 0)
    moving = lambda i, where: (0, i)
    outs = pl.pallas_call(
        functools.partial(project_kernel, (len(groups), n_rest, col_count, len(added), n_out, steps, choosing), shift_of),
        out_shape=[jax.ShapeDtypeStruct((size // n_out, total), jnp.float32)] * n_out
        + [pltpu.HBM((blocks, rows, length), jnp.float32)] * n_chosen,
        grid_spec=pltpu.PrefetchScalarGridSpec(
            num_scalar_prefetch=1,
            grid=(steps,),
            in_specs=[pl.BlockSpec((rows, tile), moving) for _ in pieces]
            + [pl.BlockSpec((total, tile), moving)] * 2
            + [pl.BlockSpec(value.shape, fixed) for value in added],
            out_specs=[pl.BlockSpec((size // n_out, total), fixed)] * n_out
            + [pl.BlockSpec((blocks, rows, tile), lambda i, where: (0, 0, i))] * n_chosen,
            scratch_shapes=[pltpu.VMEM((size, total), jnp.float32)],
        ),
        cost_estimate=pl.CostEstimate(
            flops=6 * size * total * length, bytes_accessed=4 * (2 * size + total) * length, transcendentals=0
        ),
        compiler_params=pltpu.CompilerParams(vmem_limit_bytes=32 << 20),
        name="project",
    )(where, *[outside(piece) for piece in pieces], outside(high), outside(low), *added)
    chosen = outs[n_out:]
    return outs[:n_out], [chosen[g * col_count : (g + 1) * col_count] for g in range(len(groups) if choosing else 0)]


def choose_kernel(col_count, shift_of, where_ref, *refs):
    chosen, (held_ref, in_sem, out_sem) = refs[-3 - col_count : -3], refs[-3:]
    pieces = refs[: -3 - col_count]
    blocks = len(pieces) // col_count
    shift = shift_of(where_ref[0])
    loads = [pltpu.make_async_copy(piece, held_ref.at[i], in_sem.at[i]) for i, piece in enumerate(pieces)]
    for load in loads:
        load.start()
    for load in loads:
        load.wait()
    stores = []
    for flip in range(col_count):
        for block in range(blocks):
            source = (shift ^ flip) * blocks + block
            stores.append(
                pltpu.make_async_copy(held_ref.at[source], chosen[flip].at[block], out_sem.at[len(stores)])
            )
    for store in stores:
        store.start()
    for store in stores:
        store.wait()


def choose(where, shift_of, pieces, col_count):
    rows, length = pieces[0].shape
    anywhere = pl.BlockSpec(memory_space=pltpu.HBM)
    return pl.pallas_call(
        functools.partial(choose_kernel, col_count, shift_of),
        out_shape=[pltpu.HBM((len(pieces) // col_count, rows, length), jnp.float32)] * col_count,
        grid_spec=pltpu.PrefetchScalarGridSpec(
            num_scalar_prefetch=1,
            grid=(),
            in_specs=[anywhere] * len(pieces),
            out_specs=[anywhere] * col_count,
            scratch_shapes=[
                pltpu.VMEM((len(pieces), rows, length), jnp.float32),
                pltpu.SemaphoreType.DMA((len(pieces),)),
                pltpu.SemaphoreType.DMA((len(pieces),)),
            ],
        ),
        cost_estimate=pl.CostEstimate(
            flops=1 << 28, bytes_accessed=8 * len(pieces) * rows * length, transcendentals=0
        ),
        compiler_params=pltpu.CompilerParams(vmem_limit_bytes=8 << 20),
        name="choose",
    )(where, *[outside(piece) for piece in pieces])


def factor_kernel(pair_rows, crossed_ref, factor_ref, high_ref, low_ref, whole_ref):
    count, width = factor_ref.shape[:2]
    col_count = crossed_ref.shape[0]

    def dot(left, right, axis):
        def once(first, second):
            return lax.dot_general(
                first, second, (((1,), (axis,)), ((), ())), preferred_element_type=jnp.float32
            )

        (left_high, left_low), (right_high, right_low) = halves(left), halves(right)
        return once(left_high, right_high) + once(left_high, right_low) + once(left_low, right_high)

    whole_ref[...] = jnp.zeros_like(whole_ref)
    for first in reversed(range(count)):
        at = slice(first * width, (first + 1) * width)
        factor = factor_ref[first]
        whole_ref[at, at] = factor.T
        if first < count - 1:
            inner = []
            for second in range(first + 1, count):
                pair = second * (second - 1) // 2 + first
                for col in range(col_count):
                    inner.append(crossed_ref[col, pair * pair_rows : (pair + 1) * pair_rows, :])
            inner = jnp.concatenate(inner, axis=0)
            after = (first + 1) * width
            whole_ref[after:, at] = -dot(dot(whole_ref[after:, after:], inner, 0), factor, 1)
    high, low = halves(whole_ref[...])
    high_ref[...] = high
    low_ref[...] = low


def factor(crossed, factors, pair_rows):
    count, width = factors.shape[:2]
    shape = jax.ShapeDtypeStruct((count * width, count * width), jnp.bfloat16)
    return pl.pallas_call(
        functools.partial(factor_kernel, pair_rows),
        out_shape=[shape, shape],
        scratch_shapes=[pltpu.VMEM((count * width, count * width), jnp.float32)],
        cost_estimate=pl.CostEstimate(flops=width**3 * count**3 * 4, bytes_accessed=1 << 22, transcendentals=0),
        compiler_params=pltpu.CompilerParams(vmem_limit_bytes=16 << 20),
        name="factor",
    )(crossed, factors)


def update_kernel(plan, place_of, where_ref, *refs):
    n_given, n_vector, n_before, rows = plan
    given, refs = refs[:n_given], refs[n_given:]
    vectors, refs = refs[:n_vector], refs[n_vector:]
    factor_high, factor_low, reflect_high, reflect_low = refs[:4]
    out_ref, high_ref, low_ref = refs[4 + n_before :]
    given_places, vector_places = place_of(where_ref[0])
    middle, _, inner, tile = out_ref.shape

    @pl.when(pl.program_id(0) == 0)
    def _():
        index = 0
        for ref in given:
            for block in range(ref.shape[0]):
                high, low = halves(ref[block])
                start = pl.multiple_of(given_places[index] * rows, rows)
                high_ref[pl.ds(start, rows), :] = high
                low_ref[pl.ds(start, rows), :] = low
                index += 1
        for at in chunked(high_ref.shape[1], 256):
            after = slice(at.start, None)
            update = jnp.dot(high_ref[:, after], factor_high[after, at], preferred_element_type=jnp.float32)
            update += jnp.dot(high_ref[:, after], factor_low[after, at], preferred_element_type=jnp.float32)
            update += jnp.dot(low_ref[:, after], factor_high[after, at], preferred_element_type=jnp.float32)
            high_ref[:, at], low_ref[:, at] = halves(update)

    high = high_ref[...]
    total = jnp.dot(high, reflect_high[...], preferred_element_type=jnp.float32)
    total += jnp.dot(high, reflect_low[...], preferred_element_type=jnp.float32)
    total += jnp.dot(low_ref[...], reflect_high[...], preferred_element_type=jnp.float32)
    out_ref[:, 0] = total.reshape(middle, inner, tile)
    index = 0
    for ref in vectors:
        for block in range(ref.shape[0]):
            outer, place = vector_places[index]
            at = (outer, 0, pl.ds(pl.multiple_of(place * rows, rows), rows))
            out_ref[at] = ref[block] - out_ref[at]
            index += 1


def apply_update(where, place_of, part_of, parts, middle, given, vectors, factor_parts, reflect_parts, before):
    total, length = reflect_parts[0].shape
    rows = vectors[0].shape[1]
    count = sum(value.shape[0] for value in given)
    inner = count * rows // middle
    tile = min(TILE, length)
    specs = [pl.BlockSpec(value.shape, lambda i, where: (0, 0, 0)) for value in given]
    specs += [pl.BlockSpec((value.shape[0], rows, tile), lambda i, where: (0, 0, i)) for value in vectors]
    specs += [pl.BlockSpec((total, total), lambda i, where: (0, 0))] * 2
    specs += [pl.BlockSpec((total, tile), lambda i, where: (0, i))] * 2
    specs += [pl.BlockSpec(memory_space=pltpu.HBM)] * len(before)
    return pl.pallas_call(
        functools.partial(update_kernel, (len(given), len(vectors), len(before), rows), place_of),
        out_shape=jax.ShapeDtypeStruct((middle, parts, inner, length), jnp.float32),
        grid_spec=pltpu.PrefetchScalarGridSpec(
            num_scalar_prefetch=1,
            grid=(length // tile,),
            in_specs=specs,
            out_specs=pl.BlockSpec((middle, 1, inner, tile), lambda i, where: (0, part_of(where[0]), 0, i)),
            scratch_shapes=[pltpu.VMEM((count * rows, total), jnp.bfloat16)] * 2,
        ),
        input_output_aliases={len(specs): 0} if before else {},
        cost_estimate=pl.CostEstimate(
            flops=6 * count * rows * total * length,
            bytes_accessed=4 * (2 * count * rows * length + total * length + count * rows * total),
            transcendentals=0,
        ),
        compiler_params=pltpu.CompilerParams(vmem_limit_bytes=40 << 20),
        name="apply_update",
    )(where, *given, *map(outside, vectors), *factor_parts, reflect_parts[0], outside(reflect_parts[1]), *before)


def flipped(value, amount, axis, size):
    return jnp.stack([lax.dynamic_index_in_dim(value, i ^ amount, axis, keepdims=False) for i in range(size)], axis)


def transform(vectors, reflectors, factors):
    rows, whole_length = vectors.shape
    row_count = lax.axis_size("row")
    col_count = lax.axis_size("col")
    length = whole_length // row_count
    count, own_width = reflectors.shape[:2]
    width = own_width * col_count
    per_col = row_count // col_count
    low_bits = min(LOW_BITS, per_col.bit_length() - 1)
    groups = 1 << low_bits
    middle = per_col // groups
    rest_count = col_count * middle
    row = lax.axis_index("row")
    col = lax.axis_index("col")
    where = (row * col_count + col)[None]

    def flip_row(value, bits):
        return lax.ppermute(value, "row", [(i, i ^ bits) for i in range(row_count)])

    def flip_col(value, bits):
        return lax.ppermute(value, "col", [(i, i ^ bits) for i in range(col_count)])

    reflects = [reflectors]
    for flip in range(1, col_count):
        reflects.append(flip_col(reflectors, flip))

    group_order = list(reversed(range(groups)))
    pieces = {}
    for low in group_order:
        flips = [rest * groups + low for rest in reversed(range(rest_count))]
        cuts = cut(row[None], vectors, flips, length)
        arrived = []
        for flip, piece in zip(flips, cuts):
            arrived.append(flip_row(piece, flip) if flip else piece)
        pieces[low] = arrived[::-1]

    def shift_of(w):
        return (w // col_count // per_col) ^ (w % col_count)

    half = max(groups // 2, 1)
    chosen = {}
    for low in group_order:
        chosen[low] = choose(where, shift_of, pieces[low], col_count)

    pairs = count * (count - 1) // 2
    share = -(-pairs * own_width // (row_count * 8)) * 8
    reflect_high, reflect_low, packed = prepare(where, lambda w: w % col_count, reflects, share * row_count)
    packed = packed.reshape(row_count, share, width)
    for bit in range(low_bits):
        mine = (row >> bit) & 1
        split = packed.reshape(packed.shape[0] // 2, 2, share, width)
        sent = lax.dynamic_index_in_dim(split, 1 - mine, 1, keepdims=False)
        kept = lax.dynamic_index_in_dim(split, mine, 1, keepdims=False)
        packed = kept + flip_row(sent, 1 << bit)
    rest_of = row // groups
    total = lax.dynamic_index_in_dim(packed, rest_of, 0, keepdims=False)
    for flip in range(1, rest_count):
        total = total + flip_row(lax.dynamic_index_in_dim(packed, rest_of ^ flip, 0, keepdims=False), flip * groups)
    both = [total]
    for flip in range(1, col_count):
        both.append(flip_col(total, flip))
    total = flipped(jnp.stack(both), col, 0, col_count)
    spread = [total]
    for flip in range(1, rest_count):
        spread.append(flip_row(total, flip * groups))
    spread = flipped(jnp.stack(spread), rest_of, 0, rest_count)
    for bit in reversed(range(low_bits)):
        mine = (row >> bit) & 1
        other = flip_row(spread, 1 << bit)
        spread = jnp.where(mine == 0, jnp.stack([spread, other], 1), jnp.stack([other, spread], 1))
        spread = spread.reshape(-1, col_count, share, width)
    crossed = jnp.swapaxes(spread, 0, 1).reshape(col_count, row_count * share, width)
    factor_parts = factor(crossed, factors, own_width)

    added = {low: [] for low in group_order}
    for lows in [group_order[:half]] + [[low] for low in group_order[half:]]:
        sums, _ = project(
            where,
            shift_of,
            [pieces[low] for low in lows],
            reflect_high,
            reflect_low,
            [],
            col_count,
            len(lows),
            False,
        )
        for low, value in zip(lows, sums):
            for other in added[low]:
                value = value + other
            if low:
                bit = (low & -low).bit_length() - 1
                added[low ^ (1 << bit)].append(flip_row(value, 1 << bit))
    value = value.reshape(col_count, middle, rows, count * width)
    step = middle // 2
    while step:
        value = value[:, :step] + flip_row(value[:, step:], step * groups)
        step //= 2
    sums = value[:, 0]

    moved = {}
    for low in group_order:
        for flip in range(1, col_count):
            moved[low, flip] = flip_col(chosen[low][flip], flip)

    projection = 0.0
    for high_flip in range(col_count):
        pairs_of = []
        for source_row in range(row_count):
            for source_col in range(col_count):
                high, inside = source_row // per_col, source_row % per_col
                target = (source_col * per_col + inside) * col_count + (high ^ high_flip)
                pairs_of.append((source_row * col_count + source_col, target))
        projection = projection + lax.ppermute(sums[high_flip], ("row", "col"), pairs_of)

    gathered = {}
    first_group = []
    for high_flip in range(col_count):
        for middle_flip in range(middle):
            flip = high_flip * per_col + middle_flip * groups
            first_group.append(flip_row(projection, flip) if flip else projection)
    gathered[0] = first_group
    for bit in reversed(range(low_bits)):
        for low in list(gathered):
            blocks = gathered[low]
            target = low | (1 << bit)
            if bit:
                sent = []
                for block in blocks:
                    sent.append(flip_row(block, 1 << bit))
                gathered[target] = sent
            else:
                gathered[target] = [flip_row(jnp.stack(blocks), 1)]
    gathered = {low: [b.reshape(-1, rows, count * width) for b in blocks] for low, blocks in gathered.items()}

    parts = 1
    per_part = groups // parts

    def place_of(lows):
        def places(where):
            row, col = where // col_count, where % col_count
            low_of, middle_of, high_of = row % groups, (row // groups) % middle, row // per_col
            given_places, vector_places = [], []
            for low in lows:
                inside = (low_of ^ low) % per_part
                for high_flip in range(col_count):
                    for middle_flip in range(middle):
                        given_places.append(
                            ((middle_of ^ middle_flip) * per_part + inside) * col_count + (high_of ^ high_flip)
                        )
            for flip in range(col_count):
                for low in lows:
                    inside = (low_of ^ low) % per_part
                    for middle_flip in range(middle):
                        vector_places.append((middle_of ^ middle_flip, inside * col_count + (col ^ flip)))
            return given_places, vector_places

        return places

    before = ()
    for part in range(parts):
        lows = list(range(part * per_part, (part + 1) * per_part))
        result = apply_update(
            where,
            place_of(lows),
            lambda w, part=part: ((w // col_count) % groups) // per_part ^ part,
            parts,
            middle,
            [block for low in lows for block in gathered[low]],
            [chosen[low][0] if flip == 0 else moved[low, flip] for flip in range(col_count) for low in lows],
            factor_parts,
            (reflect_high, reflect_low),
            before,
        )
        before = (result,)
    return result.reshape(row_count * rows, length)


def solution(mesh):
    return jax.shard_map(
        transform,
        mesh=mesh,
        in_specs=(P(("row", "col"), None), P(None, "col", "row"), P()),
        out_specs=P("col", "row"),
        check_vma=False,
    )
```
